256 devices in a mesh: row: 32 (over z_lo, x, core), col: 8 (over z_hi, y).
Axes of the slice: x: 4, y: 4, z: 8 (z_hi: 2, z_lo: 4; z = z_hi * 4 + z_lo), core: 2. Of those that a mesh axis runs over, the one named last changes fastest.
Arguments:
- tokens: bfloat16 [2048, 8192], P('row', 'col'), may hold values from -6 to 6
- norm_gain: bfloat16 [8192], P('col'), may hold values from 0.099609375 to 1.8984375
- gate_proj: bfloat16 [8192, 28672], P('col', 'row'), may hold values from -0.0625 to 0.0625
- up_proj: bfloat16 [8192, 28672], P('col', 'row'), may hold values from -0.0625 to 0.0625
- down_proj: bfloat16 [28672, 8192], P('row', 'col'), may hold values from -0.03125 to 0.03125
Outputs:
- mixed: bfloat16 [2048, 8192], P('row', 'col')
The draws below stay inside these ranges and needn't reach their ends.
All inputs are finite; a program needn't handle non-finite values.
Results may differ from the reference program's by a relative error of at most 0.015.
Values may be sent and summed in bfloat16 or wider, within the bound.
A program may use at most 128 MiB of HBM per device.

```python
import jax
import jax.numpy as jnp
from jax import lax

D = 8192
FF = 28672
TOKENS = 2048


def steps_of(own_key, extent, split, smallest, top_value):
    level = 1.0
    for position, blocks in split:
        draws = jax.random.uniform(jax.random.fold_in(jax.random.fold_in(own_key, 6), position), (blocks,), jnp.float32, smallest / len(split), top_value / len(split))
        level = level * jnp.repeat(jnp.exp(draws), extent[position] // blocks).reshape((-1,) + (1,) * (len(extent) - 1 - position))
    return level


def noise(stream_key, extent, width, limit, cuts=(), dtype=jnp.bfloat16):
    factor_of = steps_of(stream_key, extent, cuts, -0.22, 0.18) if cuts else 1.0
    array = jax.random.normal(stream_key, extent, jnp.float32) * width * factor_of
    return jnp.minimum(jnp.maximum(array, -limit), limit).astype(dtype)


def setup_inputs(seed: int = 0) -> dict:
    streams_of = jax.random.split(jax.random.key(seed), 6)
    tokens = noise(streams_of[0], (TOKENS, D), 1.0, 6.0, ((0, 32), (1, 8)))
    norm_gain = jnp.clip(1.0 + 0.18 * jax.random.normal(streams_of[1], (D,), jnp.float32), 0.099609375, 1.8984375).astype(jnp.bfloat16)
    gate_proj = noise(streams_of[2], (D, FF), D ** -0.5, 0.0625, ((0, 8), (1, 32)))
    up_proj = noise(streams_of[3], (D, FF), D ** -0.5, 0.0625, ((0, 8), (1, 32)))
    down_proj = noise(streams_of[4], (FF, D), FF ** -0.5, 0.03125, ((0, 32), (1, 8)))
    return {"tokens": tokens, "norm_gain": norm_gain, "gate_proj": gate_proj, "up_proj": up_proj, "down_proj": down_proj}


floor_term = 0.25

def reference(tokens, norm_gain, gate_proj, up_proj, down_proj):
    widened = tokens.astype(jnp.float32)
    square_sum = lax.optimization_barrier(jnp.sum(widened * widened, axis=1))
    row_scale = 1.0 / jnp.sqrt(square_sum / D + floor_term)
    scaled = (widened * norm_gain.astype(jnp.float32)[None, :]).astype(jnp.bfloat16)
    gate = row_scale[:, None] * jnp.dot(scaled, gate_proj, preferred_element_type=jnp.float32)
    up_value = row_scale[:, None] * jnp.dot(scaled, up_proj, preferred_element_type=jnp.float32)
    hidden = (jax.nn.silu(gate) * up_value).astype(jnp.bfloat16)
    mixed = widened + jnp.dot(hidden, down_proj, preferred_element_type=jnp.float32)
    return mixed.astype(jnp.bfloat16)
```

```python
import jax
import jax.numpy as jnp
from jax import lax
from jax.experimental import pallas as pl
from jax.experimental.pallas import tpu as pltpu
from jax.sharding import Mesh
from jax.sharding import PartitionSpec as P

D = 8192
EPS = 0.25
MESH = pl.DeviceIdType.MESH
ROW = ("zl", "x", "core")
COL = ("zh", "y")

K = 8
F32 = jnp.float32
BF16 = jnp.bfloat16

PLAN = {
    "a2": (0.0, 4.0),
    "a3": (3.0, 4.0),
    "mm": (6.0, 7.5),
    "p2": (13.0, 7.5),
    "zs": (21.0, 7.5),
    "hid": (30.0, 7.5),
    "cy": (38.0, 9.0),
    "cf": (44.0, 9.0),
    "dn": (48.0, 9.0),
    "d2": (52.0, 9.0),
    "d3": (57.0, 9.0),
    "d4": (61.0, 9.0),
}


def order():
    steps = list(PLAN)
    keyed = []
    for s, name in enumerate(steps):
        start, period = PLAN[name]
        for k in range(K):
            keyed.append((start + period * k, s, k, name))
    keyed.sort(key=lambda e: (e[0], -e[1], e[2]))
    done, out = {}, []
    for _, s, k, name in keyed:
        out.append((name, k))
    for i, (name, k) in enumerate(out):
        s = steps.index(name)
        assert s == 0 or done.get((steps[s - 1], k), i) < i
        done[(name, k)] = i
    return out


def body(
    tok, gain, gate, up, down, out,
    wgu, wd, sq, xg, part, r1, r2, zs, zr, hg, oacc, d1s, d1r, d2s, d2r, o3, d3s, d3r,
    wsem, sqS, sqR, aS, aR, bS, bR, cS, cR, dS, dR,
):
    zl, x, core, zh, y = [lax.axis_index(n) for n in ("zl", "x", "core", "zh", "y")]
    F = gate.shape[1]
    R = tok.shape[0] // K
    PR, ZR = 8 * R, 4 * R
    C = 32 * R
    col = zh * 4 + y

    def add(v, d, n):
        return lax.rem(v + d, n)

    yp, ym, y2 = add(y, 1, 4), add(y, 3, 4), add(y, 2, 4)

    w_copies = [
        pltpu.make_async_copy(gate, wgu.at[:, pl.ds(0, F)], wsem.at[0]),
        pltpu.make_async_copy(up, wgu.at[:, pl.ds(F, F)], wsem.at[1]),
        pltpu.make_async_copy(down, wd, wsem.at[2]),
    ]
    for c in w_copies:
        c.start()

    def colpeer(d):
        t = add(col, d, 8)
        return {"zh": t // 4, "y": lax.rem(t, 4)}

    peers = [colpeer(d) for d in range(1, 8)]
    peers += [{"zl": add(zl, d, 4)} for d in (1, 2, 3)]
    peers += [{"x": add(x, d, 4)} for d in (1, 2, 3)]
    peers += [{"core": 1 - core}]
    barrier = pltpu.get_barrier_semaphore()
    for p in peers:
        pl.semaphore_signal(barrier, inc=1, device_id=p, device_id_type=MESH)

    pending = []

    def send(src, dst, ss, rs, dev):
        c = pltpu.make_async_remote_copy(
            src_ref=src, dst_ref=dst, send_sem=ss, recv_sem=rs, device_id=dev, device_id_type=MESH
        )
        c.start()
        pending.append(c)

    def recv(dst, ss, rs, dev):
        pltpu.make_async_remote_copy(
            src_ref=dst, dst_ref=dst, send_sem=ss, recv_sem=rs, device_id=dev, device_id_type=MESH
        ).wait_recv()

    tw = tok[...].astype(F32)
    acc = jnp.zeros((tok.shape[0], 128), F32)
    for g in range(tok.shape[1] // 128):
        v = tw[:, g * 128 : (g + 1) * 128]
        acc = acc + v * v
    acc = jnp.concatenate([acc, jnp.zeros((128 - tok.shape[0], 128), F32)], axis=0)
    sq[col] = jnp.broadcast_to(jnp.sum(acc.T, axis=0, keepdims=True), (8, 128))
    pl.semaphore_wait(barrier, len(peers))
    for d in range(1, 8):
        send(sq.at[col], sq.at[col], sqS.at[d], sqR.at[d], colpeer(d))
    for d in range(1, 8):
        t = add(col, 8 - d, 8)
        recv(sq.at[t], sqS.at[d], sqR.at[d], colpeer(d))
    total = sq[0]
    for c in range(1, 8):
        total = total + sq[c]
    scale = 1.0 / jnp.sqrt(total / D + EPS)
    scale = jnp.broadcast_to(scale[0:1, :], (128, 128)).T[: tok.shape[0], :]
    for g in range(tok.shape[1] // 128):
        cols = slice(g * 128, (g + 1) * 128)
        xn = (tok[:, cols].astype(F32) * gain[:, cols].astype(F32) * scale).astype(BF16)
        for k in range(K):
            xg[k, core, x, zl, :, cols] = xn[k * R : (k + 1) * R]
    for k in range(K):
        mine = xg.at[k, core, x, zl]
        for d in (1, 2, 3):
            send(mine, mine, aS.at[k, d - 1], aR.at[k, d - 1], {"zl": add(zl, d, 4)})

    def a2(k):
        for d in (1, 2, 3):
            s = add(zl, 4 - d, 4)
            recv(xg.at[k, core, x, s], aS.at[k, d - 1], aR.at[k, d - 1], {"zl": s})
        mine = xg.at[k, core, x]
        for d in (1, 2, 3):
            send(mine, mine, aS.at[k, d + 2], aR.at[k, d + 2], {"x": add(x, d, 4)})

    def a3(k):
        for d in (1, 2, 3):
            s = add(x, 4 - d, 4)
            recv(xg.at[k, core, s], aS.at[k, d + 2], aR.at[k, d + 2], {"x": s})
        mine = xg.at[k, core]
        send(mine, mine, aS.at[k, 6], aR.at[k, 6], {"core": 1 - core})

    def mm(k):
        recv(xg.at[k, 1 - core], aS.at[k, 6], aR.at[k, 6], {"core": 1 - core})
        if k == 0:
            w_copies[0].wait()
            w_copies[1].wait()

        def tile(n, carry):
            cols = pl.ds(pl.multiple_of(n * 256, 256), 256)
            r = jnp.dot(
                xg[k].reshape(C, xg.shape[-1]), wgu[:, cols], preferred_element_type=F32
            )
            part[k, :, :, cols] = r.astype(BF16).reshape(4, PR, 256)
            return carry

        lax.fori_loop(0, 2 * F // 256, tile, 0)
        send(part.at[k, y2, :, pl.ds(0, F)], r1.at[k, 0], bS.at[k, 0], bR.at[k, 0], {"y": yp})
        send(part.at[k, y2, :, pl.ds(F, F)], r1.at[k, 1], bS.at[k, 1], bR.at[k, 1], {"y": ym})

    def p2(k):
        recv(r1.at[k, 0], bS.at[k, 0], bR.at[k, 0], {"y": ym})
        a = part[k, yp, :, :F].astype(F32) + r1[k, 0].astype(F32)
        part[k, yp, :, :F] = a.astype(BF16)
        send(part.at[k, yp], r2.at[k, 0], bS.at[k, 2], bR.at[k, 2], {"y": yp})
        recv(r1.at[k, 1], bS.at[k, 1], bR.at[k, 1], {"y": yp})
        a = part[k, ym, :, F:].astype(F32) + r1[k, 1].astype(F32)
        part[k, ym, :, F:] = a.astype(BF16)
        send(part.at[k, ym], r2.at[k, 1], bS.at[k, 3], bR.at[k, 3], {"y": ym})

    def ysum(k, z, cols):
        rows = pl.ds(pl.multiple_of(z * ZR, ZR), ZR)
        s = part[k, y, rows, cols].astype(F32)
        return s + r2[k, 0, rows, cols].astype(F32) + r2[k, 1, rows, cols].astype(F32)

    def zsend(k):
        recv(r2.at[k, 0], bS.at[k, 2], bR.at[k, 2], {"y": ym})
        recv(r2.at[k, 1], bS.at[k, 3], bR.at[k, 3], {"y": yp})
        for cols in (slice(0, F), slice(F, 2 * F)):
            zs[k, :, cols] = ysum(k, 1 - zh, cols).astype(BF16)
        send(zs.at[k], zr.at[k], bS.at[k, 4], bR.at[k, 4], {"zh": 1 - zh})

    def hid(k):
        recv(zr.at[k], bS.at[k, 4], bR.at[k, 4], {"zh": 1 - zh})
        g = ysum(k, zh, slice(0, F)) + zr[k, :, :F].astype(F32)
        u = ysum(k, zh, slice(F, 2 * F)) + zr[k, :, F:].astype(F32)
        hg[k, y, zh] = (jax.nn.silu(g) * u).astype(BF16)
        mine = hg.at[k, y, zh]
        send(mine, mine, cS.at[k, 0], cR.at[k, 0], {"zh": 1 - zh})

    def cy(k):
        recv(hg.at[k, y, 1 - zh], cS.at[k, 0], cR.at[k, 0], {"zh": 1 - zh})
        mine = hg.at[k, y]
        send(mine, mine, cS.at[k, 1], cR.at[k, 1], {"y": yp})
        send(mine, mine, cS.at[k, 2], cR.at[k, 2], {"y": ym})

    def cf(k):
        recv(hg.at[k, ym], cS.at[k, 1], cR.at[k, 1], {"y": ym})
        send(hg.at[k, ym, 0], hg.at[k, ym, 0], cS.at[k, 3], cR.at[k, 3], {"y": yp})
        recv(hg.at[k, yp], cS.at[k, 2], cR.at[k, 2], {"y": yp})
        send(hg.at[k, yp, 1], hg.at[k, yp, 1], cS.at[k, 4], cR.at[k, 4], {"y": ym})

    def dn(k):
        recv(hg.at[k, y2, 0], cS.at[k, 3], cR.at[k, 3], {"y": ym})
        recv(hg.at[k, y2, 1], cS.at[k, 4], cR.at[k, 4], {"y": yp})
        if k == 0:
            w_copies[2].wait()

        def tile(n, carry):
            cols = pl.ds(pl.multiple_of(n * 256, 256), 256)
            r = jnp.dot(hg[k].reshape(C, F), wd[:, cols], preferred_element_type=F32)
            both = r.reshape(2, 4, 4 * R, 256)
            oacc[k, :, :, :, cols] = both
            return carry

        lax.fori_loop(0, wd.shape[1] // 256, tile, 0)
        d1s[k] = oacc[k, 1 - core].astype(BF16)
        send(d1s.at[k], d1r.at[k], dS.at[k, 0], dR.at[k, 0], {"core": 1 - core})

    def d2(k):
        recv(d1r.at[k], dS.at[k, 0], dR.at[k, 0], {"core": 1 - core})
        for j in range(4):
            s = oacc[k, core, j] + d1r[k, j].astype(F32)
            oacc[k, core, j] = s
            d2s[k, j] = s.astype(BF16)
        for d in (1, 2, 3):
            t = add(x, d, 4)
            send(d2s.at[k, t], d2r.at[k, d - 1], dS.at[k, d], dR.at[k, d], {"x": t})

    def d3(k):
        s = oacc[k, core, x]
        for d in (1, 2, 3):
            recv(d2r.at[k, d - 1], dS.at[k, d], dR.at[k, d], {"x": add(x, d, 4)})
            s = s + d2r[k, d - 1].astype(F32)
        s = s.reshape(4, R, s.shape[-1])
        o3[k] = s
        d3s[k] = s.astype(BF16)
        for d in (1, 2, 3):
            t = add(zl, d, 4)
            send(d3s.at[k, t], d3r.at[k, d - 1], dS.at[k, d + 3], dR.at[k, d + 3], {"zl": t})

    def d4(k):
        s = tok[k * R : (k + 1) * R, :].astype(F32) + o3[k, zl]
        for d in (1, 2, 3):
            recv(d3r.at[k, d - 1], dS.at[k, d + 3], dR.at[k, d + 3], {"zl": add(zl, d, 4)})
            s = s + d3r[k, d - 1].astype(F32)
        out[k * R : (k + 1) * R, :] = s.astype(BF16)

    ops = dict(a2=a2, a3=a3, mm=mm, p2=p2, zs=zsend, hid=hid, cy=cy, cf=cf, dn=dn, d2=d2, d3=d3, d4=d4)
    for name, k in order():
        ops[name](k)
    for c in pending:
        c.wait_send()


def shards(tokens, norm_gain, gate_proj, up_proj, down_proj):
    T, DB = tokens.shape
    F = gate_proj.shape[1]
    R = T // K
    PR, ZR = 8 * R, 4 * R
    vmem = pl.BlockSpec(memory_space=pltpu.VMEM)
    hbm = pl.BlockSpec(memory_space=pl.ANY)
    dma = pltpu.SemaphoreType.DMA
    return pl.pallas_call(
        body,
        out_shape=jax.ShapeDtypeStruct((T, DB), BF16),
        in_specs=[vmem, vmem, hbm, hbm, hbm],
        out_specs=vmem,
        scratch_shapes=[
            pltpu.VMEM((DB, 2 * F), BF16),
            pltpu.VMEM((F, DB), BF16),
            pltpu.VMEM((8, 8, 128), F32),
            pltpu.VMEM((K, 2, 4, 4, R, DB), BF16),
            pltpu.VMEM((K, 4, PR, 2 * F), BF16),
            pltpu.VMEM((K, 2, PR, F), BF16),
            pltpu.VMEM((K, 2, PR, 2 * F), BF16),
            pltpu.VMEM((K, ZR, 2 * F), BF16),
            pltpu.VMEM((K, ZR, 2 * F), BF16),
            pltpu.VMEM((K, 4, 2, ZR, F), BF16),
            pltpu.VMEM((K, 2, 4, 4 * R, DB), F32),
            pltpu.VMEM((K, 4, 4 * R, DB), BF16),
            pltpu.VMEM((K, 4, 4 * R, DB), BF16),
            pltpu.VMEM((K, 4, 4 * R, DB), BF16),
            pltpu.VMEM((K, 3, 4 * R, DB), BF16),
            pltpu.VMEM((K, 4, R, DB), F32),
            pltpu.VMEM((K, 4, R, DB), BF16),
            pltpu.VMEM((K, 3, R, DB), BF16),
            dma((3,)),
            dma((8,)),
            dma((8,)),
            dma((K, 7)),
            dma((K, 7)),
            dma((K, 5)),
            dma((K, 5)),
            dma((K, 5)),
            dma((K, 5)),
            dma((K, 7)),
            dma((K, 7)),
        ],
        compiler_params=pltpu.CompilerParams(
            collective_id=0, has_side_effects=True, vmem_limit_bytes=60 * 2**20
        ),
        name="ffn",
    )(tokens, norm_gain.reshape(1, -1), gate_proj, up_proj, down_proj)


def solution(mesh):
    split = Mesh(mesh.devices.reshape(4, 4, 2, 2, 4), ROW + COL)
    return jax.shard_map(
        shards,
        mesh=split,
        in_specs=(P(ROW, COL), P(COL), P(COL, ROW), P(COL, ROW), P(ROW, COL)),
        out_specs=P(ROW, COL),
        check_vma=False,
    )
```

```python
import jax
import jax.numpy as jnp
from jax import lax
from jax.experimental import pallas as pl
from jax.experimental.pallas import tpu as pltpu
from jax.sharding import Mesh
from jax.sharding import PartitionSpec as P

D = 8192
EPS = 0.25
MESH = pl.DeviceIdType.MESH
ROW = ("zl", "x", "core")
COL = ("zh", "y")

K = 8
F32 = jnp.float32
BF16 = jnp.bfloat16

STEPS = ("a2", "a3", "mm", "p2", "zs", "hid", "cy", "cf", "dn", "d2", "d3", "d4", "s1", "s2", "s3", "s4")
ORDER = (
    0, 1, 4, 16, 2, 32, 33, 17, 34, 48, 3, 192, 6, 20, 49, 18, 35, 208, 50, 37,
    41, 64, 7, 5, 19, 224, 40, 65, 36, 53, 240, 80, 57, 23, 21, 66, 43, 38, 52, 69,
    81, 51, 42, 82, 56, 54, 59, 67, 73, 68, 97, 39, 85, 58, 72, 83, 22, 44, 113, 84,
    55, 75, 45, 70, 60, 71, 129, 61, 96, 101, 74, 98, 47, 100, 89, 91, 112, 88, 76, 99,
    87, 90, 86, 46, 63, 77, 128, 62, 117, 114, 116, 103, 79, 115, 78, 133, 102, 130, 105, 104,
    144, 106, 132, 93, 119, 146, 92, 95, 131, 121, 118, 94, 145, 107, 120, 108, 135, 134, 162, 122,
    109, 147, 136, 123, 110, 137, 148, 124, 125, 111, 138, 139, 149, 126, 140, 127, 141, 150, 163, 164,
    160, 142, 143, 151, 179, 165, 161, 166, 176, 167, 177, 181, 182, 180, 178, 183,
)


def own_half(j):
    return (j % 2 == 0) == (j // 2 < K // 2)


def body(
    tok_hbm, gain_hbm, gate, up, down, out,
    tok, gain, wgu, wd, sq, sg, sc, xg, part, r1, r2, zs, zr, hg, oacc, d1s, d1r, d2s, d2r, o3, d3s, d3r,
    wsem, sqS, sqR, eS, eR, aS, aR, bS, bR, cS, cR, dS, dR,
):
    zl, x, core, zh, y = [lax.axis_index(n) for n in ("zl", "x", "core", "zh", "y")]
    F = gate.shape[1]
    R = tok.shape[0] // K
    PR, ZR, C = 4 * R, 2 * R, 16 * R
    col = zh * 4 + y

    def add(v, d, n):
        return lax.rem(v + d, n)

    yp, ym, y2 = add(y, 1, 4), add(y, 3, 4), add(y, 2, 4)

    t_copy = pltpu.make_async_copy(tok_hbm, tok, wsem.at[3])
    t_copy.start()
    g_copy = pltpu.make_async_copy(gain_hbm, gain, wsem.at[4])
    g_copy.start()
    w_copies = [
        pltpu.make_async_copy(gate, wgu.at[:, pl.ds(0, F)], wsem.at[0]),
        pltpu.make_async_copy(up, wgu.at[:, pl.ds(F, F)], wsem.at[1]),
        pltpu.make_async_copy(down, wd, wsem.at[2]),
    ]
    for c in w_copies:
        c.start()

    def colpeer(d):
        t = add(col, d, 8)
        return {"zh": t // 4, "y": lax.rem(t, 4)}

    peers = [colpeer(d) for d in range(1, 8)]
    peers += [{"zl": add(zl, d, 4)} for d in (1, 2, 3)]
    peers += [{"x": add(x, d, 4)} for d in (1, 2, 3)]
    peers += [{"core": 1 - core}]
    barrier = pltpu.get_barrier_semaphore()
    for p in peers:
        pl.semaphore_signal(barrier, inc=1, device_id=p, device_id_type=MESH)

    pending = []

    def send(src, dst, ss, rs, dev):
        c = pltpu.make_async_remote_copy(
            src_ref=src, dst_ref=dst, send_sem=ss, recv_sem=rs, device_id=dev, device_id_type=MESH
        )
        c.start()
        pending.append(c)

    def recv(dst, ss, rs, dev):
        pltpu.make_async_remote_copy(
            src_ref=dst, dst_ref=dst, send_sem=ss, recv_sem=rs, device_id=dev, device_id_type=MESH
        ).wait_recv()

    t_copy.wait()
    g_copy.wait()
    gain_row = gain[...].reshape(1, -1).astype(F32)
    acc = jnp.zeros((tok.shape[0], 128), F32)
    for g in range(tok.shape[1] // 128):
        cols = slice(g * 128, (g + 1) * 128)
        v = tok[:, cols].astype(F32)
        acc = acc + v * v
        v = (v * gain_row[:, cols]).astype(BF16)
        for k in range(K):
            xg[k, core, x, zl, :, cols] = v[k * R : (k + 1) * R]
    acc = jnp.concatenate([acc, jnp.zeros((128 - tok.shape[0], 128), F32)], axis=0)
    sq[col] = jnp.broadcast_to(jnp.sum(acc.T, axis=0, keepdims=True), (8, 128))
    pl.semaphore_wait(barrier, len(peers))

    def a1(k):
        mine = xg.at[k, core, x, zl]
        for d in (1, 2, 3):
            send(mine, mine, aS.at[k, d - 1], aR.at[k, d - 1], {"zl": add(zl, d, 4)})

    a1(0)
    for d in range(1, 8):
        send(sq.at[col], sq.at[col], sqS.at[d], sqR.at[d], colpeer(d))
    for k in range(1, K):
        a1(k)

    def s1(_):
        for d in range(1, 8):
            t = add(col, 8 - d, 8)
            recv(sq.at[t], sqS.at[d], sqR.at[d], colpeer(d))
        total = sq[0]
        for c in range(1, 8):
            total = total + sq[c]
        sg[core, x, zl] = 1.0 / jnp.sqrt(total / D + EPS)
        mine = sg.at[core, x, zl]
        for d in (1, 2, 3):
            send(mine, mine, eS.at[d - 1], eR.at[d - 1], {"zl": add(zl, d, 4)})

    def s2(_):
        for d in (1, 2, 3):
            s = add(zl, 4 - d, 4)
            recv(sg.at[core, x, s], eS.at[d - 1], eR.at[d - 1], {"zl": s})
        mine = sg.at[core, x]
        for d in (1, 2, 3):
            send(mine, mine, eS.at[d + 2], eR.at[d + 2], {"x": add(x, d, 4)})

    def s3(_):
        for d in (1, 2, 3):
            s = add(x, 4 - d, 4)
            recv(sg.at[core, s], eS.at[d + 2], eR.at[d + 2], {"x": s})
        mine = sg.at[core]
        send(mine, mine, eS.at[6], eR.at[6], {"core": 1 - core})

    def s4(_):
        recv(sg.at[1 - core], eS.at[6], eR.at[6], {"core": 1 - core})
        for h in (0, 1):
            for i in (0, 1):
                v = jnp.broadcast_to(sg[h, y, 2 * zh + i][0:1, :], (128, 128)).T
                sc[h, :, i] = v[: K * R, :].reshape(K, R, 128)

    def a2(k):
        for d in (1, 2, 3):
            s = add(zl, 4 - d, 4)
            recv(xg.at[k, core, x, s], aS.at[k, d - 1], aR.at[k, d - 1], {"zl": s})
        mine = xg.at[k, core, x]
        for d in (1, 2, 3):
            send(mine, mine, aS.at[k, d + 2], aR.at[k, d + 2], {"x": add(x, d, 4)})

    def a3(k):
        for d in (1, 2, 3):
            s = add(x, 4 - d, 4)
            recv(xg.at[k, core, s], aS.at[k, d + 2], aR.at[k, d + 2], {"x": s})
        mine = xg.at[k, core]
        send(mine, mine, aS.at[k, 6], aR.at[k, 6], {"core": 1 - core})

    def mm(j):
        k = j // 2
        half = core if own_half(j) else 1 - core
        if not own_half(j):
            recv(xg.at[k, half], aS.at[k, 6], aR.at[k, 6], {"core": 1 - core})
        if not weights:
            weights.append(True)
            w_copies[0].wait()
            w_copies[1].wait()

        def tile(n, carry):
            cols = pl.ds(pl.multiple_of(n * 256, 256), 256)
            r = jnp.dot(
                xg[k, half].reshape(C, xg.shape[-1]), wgu[:, cols], preferred_element_type=F32
            )
            part[j, :, :, cols] = r.astype(BF16).reshape(4, PR, 256)
            return carry

        lax.fori_loop(0, 2 * F // 256, tile, 0, unroll=True)
        send(part.at[j, y2, :, pl.ds(0, F)], r1.at[j, 0], bS.at[j, 0], bR.at[j, 0], {"y": yp})
        send(part.at[j, y2, :, pl.ds(F, F)], r1.at[j, 1], bS.at[j, 1], bR.at[j, 1], {"y": ym})

    def p2(j):
        recv(r1.at[j, 0], bS.at[j, 0], bR.at[j, 0], {"y": ym})
        a = part[j, yp, :, :F].astype(F32) + r1[j, 0].astype(F32)
        part[j, yp, :, :F] = a.astype(BF16)
        send(part.at[j, yp], r2.at[j, 0], bS.at[j, 2], bR.at[j, 2], {"y": yp})
        recv(r1.at[j, 1], bS.at[j, 1], bR.at[j, 1], {"y": yp})
        a = part[j, ym, :, F:].astype(F32) + r1[j, 1].astype(F32)
        part[j, ym, :, F:] = a.astype(BF16)
        send(part.at[j, ym], r2.at[j, 1], bS.at[j, 3], bR.at[j, 3], {"y": ym})

    def ysum(j, z, cols):
        rows = pl.ds(pl.multiple_of(z * ZR, ZR), ZR)
        s = part[j, y, rows, cols].astype(F32)
        return s + r2[j, 0, rows, cols].astype(F32) + r2[j, 1, rows, cols].astype(F32)

    def zsend(j):
        recv(r2.at[j, 0], bS.at[j, 2], bR.at[j, 2], {"y": ym})
        recv(r2.at[j, 1], bS.at[j, 3], bR.at[j, 3], {"y": yp})
        for cols in (slice(0, F), slice(F, 2 * F)):
            zs[j, :, cols] = ysum(j, 1 - zh, cols).astype(BF16)
        send(zs.at[j], zr.at[j], bS.at[j, 4], bR.at[j, 4], {"zh": 1 - zh})

    def hid(j):
        recv(zr.at[j], bS.at[j, 4], bR.at[j, 4], {"zh": 1 - zh})
        g = ysum(j, zh, slice(0, F)) + zr[j, :, :F].astype(F32)
        u = ysum(j, zh, slice(F, 2 * F)) + zr[j, :, F:].astype(F32)
        k = j // 2
        scale = sc[core if own_half(j) else 1 - core, k].reshape(ZR, 128)[:, 0:1]
        g = g * scale
        u = u * scale
        hg[j, y, zh] = (jax.nn.silu(g) * u).astype(BF16)
        mine = hg.at[j, y, zh]
        send(mine, mine, cS.at[j, 0], cR.at[j, 0], {"zh": 1 - zh})

    def cy(j):
        recv(hg.at[j, y, 1 - zh], cS.at[j, 0], cR.at[j, 0], {"zh": 1 - zh})
        mine = hg.at[j, y]
        send(mine, mine, cS.at[j, 1], cR.at[j, 1], {"y": yp})
        send(mine, mine, cS.at[j, 2], cR.at[j, 2], {"y": ym})

    def cf(j):
        recv(hg.at[j, ym], cS.at[j, 1], cR.at[j, 1], {"y": ym})
        send(hg.at[j, ym, 0], hg.at[j, ym, 0], cS.at[j, 3], cR.at[j, 3], {"y": yp})
        recv(hg.at[j, yp], cS.at[j, 2], cR.at[j, 2], {"y": yp})
        send(hg.at[j, yp, 1], hg.at[j, yp, 1], cS.at[j, 4], cR.at[j, 4], {"y": ym})

    def dn(j):
        k = j // 2
        recv(hg.at[j, y2, 0], cS.at[j, 3], cR.at[j, 3], {"y": ym})
        recv(hg.at[j, y2, 1], cS.at[j, 4], cR.at[j, 4], {"y": yp})
        if len(weights) == 1:
            weights.append(True)
            w_copies[2].wait()

        def tile(n, carry):
            cols = pl.ds(pl.multiple_of(n * 256, 256), 256)
            r = jnp.dot(hg[j].reshape(C, F), wd[:, cols], preferred_element_type=F32)
            r = r.reshape(4, 4 * R, 256)
            if own_half(j):
                oacc[k, :, :, cols] = r
            else:
                d1s[k, :, :, cols] = r.astype(BF16)
            return carry

        lax.fori_loop(0, wd.shape[1] // 256, tile, 0, unroll=True)
        if not own_half(j):
            send(d1s.at[k], d1r.at[k], dS.at[k, 0], dR.at[k, 0], {"core": 1 - core})

    def d2(k):
        recv(d1r.at[k], dS.at[k, 0], dR.at[k, 0], {"core": 1 - core})
        for i in range(4):
            s = oacc[k, i] + d1r[k, i].astype(F32)
            oacc[k, i] = s
            d2s[k, i] = s.astype(BF16)
        for d in (1, 2, 3):
            t = add(x, d, 4)
            send(d2s.at[k, t], d2r.at[k, d - 1], dS.at[k, d], dR.at[k, d], {"x": t})

    def d3(k):
        s = oacc[k, x]
        for d in (1, 2, 3):
            recv(d2r.at[k, d - 1], dS.at[k, d], dR.at[k, d], {"x": add(x, d, 4)})
            s = s + d2r[k, d - 1].astype(F32)
        s = s.reshape(4, R, s.shape[-1])
        o3[k] = s
        d3s[k] = s.astype(BF16)
        for d in (1, 2, 3):
            t = add(zl, d, 4)
            send(d3s.at[k, t], d3r.at[k, d - 1], dS.at[k, d + 3], dR.at[k, d + 3], {"zl": t})

    def d4(k):
        s = tok[k * R : (k + 1) * R, :].astype(F32) + o3[k, zl]
        for d in (1, 2, 3):
            recv(d3r.at[k, d - 1], dS.at[k, d + 3], dR.at[k, d + 3], {"zl": add(zl, d, 4)})
            s = s + d3r[k, d - 1].astype(F32)
        out[k * R : (k + 1) * R, :] = s.astype(BF16)

    weights = []
    ops = (a2, a3, mm, p2, zsend, hid, cy, cf, dn, d2, d3, d4, s1, s2, s3, s4)
    for o in ORDER:
        ops[o // 16](o % 16)
    for c in pending:
        c.wait_send()


def shards(tokens, norm_gain, gate_proj, up_proj, down_proj):
    T, DB = tokens.shape
    F = gate_proj.shape[1]
    R = T // K
    PR, ZR, H = 4 * R, 2 * R, 2 * K
    vmem = pl.BlockSpec(memory_space=pltpu.VMEM)
    hbm = pl.BlockSpec(memory_space=pl.ANY)
    dma = pltpu.SemaphoreType.DMA
    return pl.pallas_call(
        body,
        out_shape=jax.ShapeDtypeStruct((T, DB), BF16),
        in_specs=[hbm, hbm, hbm, hbm, hbm],
        out_specs=vmem,
        scratch_shapes=[
            pltpu.VMEM((T, DB), BF16),
            pltpu.VMEM((DB,), BF16),
            pltpu.VMEM((DB, 2 * F), BF16),
            pltpu.VMEM((F, DB), BF16),
            pltpu.VMEM((8, 8, 128), F32),
            pltpu.VMEM((2, 4, 4, 8, 128), F32),
            pltpu.VMEM((2, K, 2, R, 128), F32),
            pltpu.VMEM((K, 2, 4, 4, R, DB), BF16),
            pltpu.VMEM((H, 4, PR, 2 * F), BF16),
            pltpu.VMEM((H, 2, PR, F), BF16),
            pltpu.VMEM((H, 2, PR, 2 * F), BF16),
            pltpu.VMEM((H, ZR, 2 * F), BF16),
            pltpu.VMEM((H, ZR, 2 * F), BF16),
            pltpu.VMEM((H, 4, 2, ZR, F), BF16),
            pltpu.VMEM((K, 4, 4 * R, DB), F32),
            pltpu.VMEM((K, 4, 4 * R, DB), BF16),
            pltpu.VMEM((K, 4, 4 * R, DB), BF16),
            pltpu.VMEM((K, 4, 4 * R, DB), BF16),
            pltpu.VMEM((K, 3, 4 * R, DB), BF16),
            pltpu.VMEM((K, 4, R, DB), F32),
            pltpu.VMEM((K, 4, R, DB), BF16),
            pltpu.VMEM((K, 3, R, DB), BF16),
            dma((5,)),
            dma((8,)),
            dma((8,)),
            dma((7,)),
            dma((7,)),
            dma((K, 7)),
            dma((K, 7)),
            dma((H, 5)),
            dma((H, 5)),
            dma((H, 5)),
            dma((H, 5)),
            dma((K, 7)),
            dma((K, 7)),
        ],
        compiler_params=pltpu.CompilerParams(
            collective_id=0, has_side_effects=True, vmem_limit_bytes=60 * 2**20
        ),
        name="ffn",
    )(tokens, norm_gain, gate_proj, up_proj, down_proj)


def solution(mesh):
    split = Mesh(mesh.devices.reshape(4, 4, 2, 2, 4), ROW + COL)
    return jax.shard_map(
        shards,
        mesh=split,
        in_specs=(P(ROW, COL), P(COL), P(COL, ROW), P(COL, ROW), P(ROW, COL)),
        out_specs=P(ROW, COL),
        check_vma=False,
    )
```

```python
import jax
import jax.numpy as jnp
from jax import lax
from jax.experimental import pallas as pl
from jax.experimental.pallas import tpu as pltpu
from jax.sharding import Mesh
from jax.sharding import PartitionSpec as P

D = 8192
EPS = 0.25
MESH = pl.DeviceIdType.MESH
ROW = ("zl", "x", "core")
COL = ("zh", "y")

G = 2
DX = ((0, 1, 3, 2), (2, 3, 1, 0))
F32 = jnp.float32
BF16 = jnp.bfloat16

STEPS = (
    "a1", "a2", "a3", "mm", "p2", "zs", "hid", "cy", "cf", "dn", "d2", "d3", "d4", "s1", "s2", "s3", "s4",
)
ORDER = (
    1, 16, 48, 49, 64, 33, 34, 65, 208, 52, 17, 53, 51, 68, 35, 50, 55, 67, 69, 81,
    54, 84, 37, 71, 224, 38, 36, 83, 66, 57, 80, 58, 87, 59, 70, 85, 82, 240, 62, 74,
    256, 97, 103, 56, 75, 86, 100, 98, 60, 61, 99, 72, 90, 63, 102, 76, 119, 77, 91, 78,
    101, 79, 106, 92, 107, 93, 115, 73, 88, 94, 122, 114, 108, 131, 89, 123, 118, 104, 96, 109,
    135, 130, 139, 116, 147, 138, 134, 95, 117, 151, 132, 105, 146, 113, 161, 124, 133, 150, 163, 148,
    110, 125, 155, 154, 111, 120, 140, 149, 165, 121, 162, 141, 136, 126, 156, 137, 112, 129, 157, 152,
    166, 127, 153, 128, 164, 142, 145, 143, 144, 160, 176, 158, 159, 167, 177, 192, 193,
)


def own_half(j):
    return (j % 2 == 0) == (j < 8)


def body(
    tok_hbm, gain_hbm, gate, up, down, out,
    tok, gain, wgu, wd, sq, sg, sc, xg, part, r1, r2, zs, zr, hg, oacc, d1s, d1r, d2s, d2r, o3, d3s, d3r,
    wsem, sqS, sqR, eS, eR, aS, aR, bS, bR, cS, cR, dS, dR, fS, fR,
):
    zl, x, core, zh, y = [lax.axis_index(n) for n in ("zl", "x", "core", "zh", "y")]
    F = gate.shape[1]
    Q = tok.shape[0] // G
    PR, ZR, C = Q, Q // 2, 4 * Q
    col = zh * 4 + y

    def add(v, d, n):
        return lax.rem(v + d, n)

    yp, ym, y2 = add(y, 1, 4), add(y, 3, 4), add(y, 2, 4)

    t_copy = pltpu.make_async_copy(tok_hbm, tok, wsem.at[3])
    t_copy.start()
    g_copy = pltpu.make_async_copy(gain_hbm, gain, wsem.at[4])
    g_copy.start()
    w_copies = [
        pltpu.make_async_copy(gate, wgu.at[:, pl.ds(0, F)], wsem.at[0]),
        pltpu.make_async_copy(up, wgu.at[:, pl.ds(F, F)], wsem.at[1]),
        pltpu.make_async_copy(down, wd, wsem.at[2]),
    ]
    for c in w_copies:
        c.start()

    def colpeer(d):
        t = add(col, d, 8)
        return {"zh": t // 4, "y": lax.rem(t, 4)}

    peers = [colpeer(d) for d in range(1, 8)]
    peers += [{"zl": add(zl, d, 4)} for d in (1, 2, 3)]
    peers += [{"x": add(x, d, 4)} for d in (1, 2, 3)]
    peers += [{"core": 1 - core}]
    barrier = pltpu.get_barrier_semaphore()
    for p in peers:
        pl.semaphore_signal(barrier, inc=1, device_id=p, device_id_type=MESH)

    pending = []

    def send(src, dst, ss, rs, dev):
        c = pltpu.make_async_remote_copy(
            src_ref=src, dst_ref=dst, send_sem=ss, recv_sem=rs, device_id=dev, device_id_type=MESH
        )
        c.start()
        pending.append(c)

    def recv(dst, ss, rs, dev):
        pltpu.make_async_remote_copy(
            src_ref=dst, dst_ref=dst, send_sem=ss, recv_sem=rs, device_id=dev, device_id_type=MESH
        ).wait_recv()

    t_copy.wait()
    g_copy.wait()
    gain_row = gain[...].reshape(1, -1).astype(F32)
    acc = jnp.zeros((tok.shape[0], 128), F32)
    for g in range(tok.shape[1] // 128):
        cols = slice(g * 128, (g + 1) * 128)
        v = tok[:, cols].astype(F32)
        acc = acc + v * v
        v = (v * gain_row[:, cols]).astype(BF16)
        for g2 in range(G):
            xg[g2, x, core, zl, :, cols] = v[g2 * Q : (g2 + 1) * Q]
    acc = jnp.concatenate([acc, jnp.zeros((128 - tok.shape[0], 128), F32)], axis=0)
    sq[col] = jnp.broadcast_to(jnp.sum(acc.T, axis=0, keepdims=True), (8, 128))
    pl.semaphore_wait(barrier, len(peers))

    def xsend(g, d, b):
        mine = xg.at[g, x, core, add(zl, b, 4)]
        i = 3 + 4 * (d - 1) + b
        send(mine, mine, aS.at[g, i], aR.at[g, i], {"x": add(x, d, 4)})

    def a1(g):
        mine = xg.at[g, x, core, zl]
        for d in (1, 2, 3):
            send(mine, mine, aS.at[g, d - 1], aR.at[g, d - 1], {"zl": add(zl, d, 4)})
        for d in (1, 3, 2):
            xsend(g, d, 0)

    a1(0)
    for d in range(1, 8):
        send(sq.at[col], sq.at[col], sqS.at[d], sqR.at[d], colpeer(d))

    def s1(_):
        for d in range(1, 8):
            t = add(col, 8 - d, 8)
            recv(sq.at[t], sqS.at[d], sqR.at[d], colpeer(d))
        total = sq[0]
        for c in range(1, 8):
            total = total + sq[c]
        sg[core, x, zl] = 1.0 / jnp.sqrt(total / D + EPS)
        mine = sg.at[core, x, zl]
        for d in (1, 2, 3):
            send(mine, mine, eS.at[d - 1], eR.at[d - 1], {"zl": add(zl, d, 4)})

    def s2(_):
        for d in (1, 2, 3):
            s = add(zl, 4 - d, 4)
            recv(sg.at[core, x, s], eS.at[d - 1], eR.at[d - 1], {"zl": s})
        mine = sg.at[core, x]
        for d in (1, 2, 3):
            send(mine, mine, eS.at[d + 2], eR.at[d + 2], {"x": add(x, d, 4)})

    def s3(_):
        for d in (1, 2, 3):
            s = add(x, 4 - d, 4)
            recv(sg.at[core, s], eS.at[d + 2], eR.at[d + 2], {"x": s})
        mine = sg.at[core]
        send(mine, mine, eS.at[6], eR.at[6], {"core": 1 - core})

    def s4(_):
        recv(sg.at[1 - core], eS.at[6], eR.at[6], {"core": 1 - core})
        for h in (0, 1):
            for dx in range(4):
                v = jnp.broadcast_to(sg[h, add(x, dx, 4), y][0:1, :], (128, 128)).T
                sc[h, dx] = v[: G * Q, :].reshape(G, 2, ZR, 128)

    def a2(g):
        for d in (1, 2, 3):
            t = add(zl, 4 - d, 4)
            recv(xg.at[g, x, core, t], aS.at[g, d - 1], aR.at[g, d - 1], {"zl": t})
        mine = xg.at[g, x, core]
        send(mine, mine, aS.at[g, 15], aR.at[g, 15], {"core": 1 - core})
        for b in (1, 2, 3):
            for d in (1, 3, 2):
                xsend(g, d, b)

    def a3(c):
        g, dx = c // 4, DX[c // 4][c % 4]
        src, d = add(x, dx, 4), 4 - dx
        for b in range(4):
            i = 3 + 4 * (d - 1) + b
            recv(xg.at[g, src, core, add(zl, b, 4)], aS.at[g, i], aR.at[g, i], {"x": src})
        mine = xg.at[g, src, core]
        send(mine, mine, aS.at[g, 15 + dx], aR.at[g, 15 + dx], {"core": 1 - core})

    def mm(j):
        g, dx = j // 8, DX[j // 8][j // 2 % 4]
        src = add(x, dx, 4)
        half = core if own_half(j) else 1 - core
        if not own_half(j):
            recv(xg.at[g, src, half], aS.at[g, 15 + dx], aR.at[g, 15 + dx], {"core": 1 - core})
        if not weights:
            weights.append(True)
            w_copies[0].wait()
            w_copies[1].wait()

        def tile(n, carry):
            cols = pl.ds(pl.multiple_of(n * 256, 256), 256)
            r = jnp.dot(
                xg[g, src, half].reshape(C, xg.shape[-1]), wgu[:, cols], preferred_element_type=F32
            )
            part[j, :, :, cols] = r.astype(BF16).reshape(4, PR, 256)
            return carry

        lax.fori_loop(0, 2 * F // 256, tile, 0, unroll=True)
        send(part.at[j, y2, :, pl.ds(0, F)], r1.at[j, 0], bS.at[j, 0], bR.at[j, 0], {"y": yp})
        send(part.at[j, y2, :, pl.ds(F, F)], r1.at[j, 1], bS.at[j, 1], bR.at[j, 1], {"y": ym})

    def p2(j):
        recv(r1.at[j, 0], bS.at[j, 0], bR.at[j, 0], {"y": ym})
        a = part[j, yp, :, :F].astype(F32) + r1[j, 0].astype(F32)
        part[j, yp, :, :F] = a.astype(BF16)
        send(part.at[j, yp], r2.at[j, 0], bS.at[j, 2], bR.at[j, 2], {"y": yp})
        recv(r1.at[j, 1], bS.at[j, 1], bR.at[j, 1], {"y": yp})
        a = part[j, ym, :, F:].astype(F32) + r1[j, 1].astype(F32)
        part[j, ym, :, F:] = a.astype(BF16)
        send(part.at[j, ym], r2.at[j, 1], bS.at[j, 3], bR.at[j, 3], {"y": ym})

    def ysum(j, z, cols):
        rows = pl.ds(pl.multiple_of(z * ZR, ZR), ZR)
        s = part[j, y, rows, cols].astype(F32)
        return s + r2[j, 0, rows, cols].astype(F32) + r2[j, 1, rows, cols].astype(F32)

    def zsend(j):
        recv(r2.at[j, 0], bS.at[j, 2], bR.at[j, 2], {"y": ym})
        recv(r2.at[j, 1], bS.at[j, 3], bR.at[j, 3], {"y": yp})
        for cols in (slice(0, F), slice(F, 2 * F)):
            zs[j, :, cols] = ysum(j, 1 - zh, cols).astype(BF16)
        send(zs.at[j], zr.at[j], bS.at[j, 4], bR.at[j, 4], {"zh": 1 - zh})

    def hid(j):
        recv(zr.at[j], bS.at[j, 4], bR.at[j, 4], {"zh": 1 - zh})
        g = ysum(j, zh, slice(0, F)) + zr[j, :, :F].astype(F32)
        u = ysum(j, zh, slice(F, 2 * F)) + zr[j, :, F:].astype(F32)
        g2, dx = j // 8, DX[j // 8][j // 2 % 4]
        scale = sc[core if own_half(j) else 1 - core, dx, g2, zh][:, 0:1]
        g = g * scale
        u = u * scale
        hg[j, y, zh] = (jax.nn.silu(g) * u).astype(BF16)
        mine = hg.at[j, y, zh]
        send(mine, mine, cS.at[j, 0], cR.at[j, 0], {"zh": 1 - zh})

    def cy(j):
        recv(hg.at[j, y, 1 - zh], cS.at[j, 0], cR.at[j, 0], {"zh": 1 - zh})
        mine = hg.at[j, y]
        send(mine, mine, cS.at[j, 1], cR.at[j, 1], {"y": yp})
        send(mine, mine, cS.at[j, 2], cR.at[j, 2], {"y": ym})

    def cf(j):
        recv(hg.at[j, ym], cS.at[j, 1], cR.at[j, 1], {"y": ym})
        send(hg.at[j, ym, 0], hg.at[j, ym, 0], cS.at[j, 3], cR.at[j, 3], {"y": yp})
        recv(hg.at[j, yp], cS.at[j, 2], cR.at[j, 2], {"y": yp})
        send(hg.at[j, yp, 1], hg.at[j, yp, 1], cS.at[j, 4], cR.at[j, 4], {"y": ym})

    def dn(j):
        k = j // 2
        recv(hg.at[j, y2, 0], cS.at[j, 3], cR.at[j, 3], {"y": ym})
        recv(hg.at[j, y2, 1], cS.at[j, 4], cR.at[j, 4], {"y": yp})
        if len(weights) == 1:
            weights.append(True)
            w_copies[2].wait()

        def tile(n, carry):
            cols = pl.ds(pl.multiple_of(n * 256, 256), 256)
            r = jnp.dot(hg[j].reshape(C, F), wd[:, cols], preferred_element_type=F32)
            r = r.reshape(4, Q, 256)
            if own_half(j):
                oacc[k, :, :, cols] = r
            else:
                d1s[k, :, :, cols] = r.astype(BF16)
            return carry

        lax.fori_loop(0, wd.shape[1] // 256, tile, 0, unroll=True)
        if not own_half(j):
            send(d1s.at[k], d1r.at[k], dS.at[k, 0], dR.at[k, 0], {"core": 1 - core})

    def d2(c):
        dx = DX[c // 4][c % 4]
        recv(d1r.at[c], dS.at[c, 0], dR.at[c, 0], {"core": 1 - core})
        for i in range(4):
            s = oacc[c, i] + d1r[c, i].astype(F32)
            if dx:
                d2s[c, i] = s.astype(BF16)
            else:
                oacc[c, i] = s
        if dx:
            send(d2s.at[c], d2r.at[c], dS.at[c, 1], dR.at[c, 1], {"x": add(x, dx, 4)})

    def d3(g):
        mine = 4 * g + DX[g].index(0)
        others = [4 * g + i for i in range(4) if DX[g][i]]
        for c in others:
            recv(d2r.at[c], dS.at[c, 1], dR.at[c, 1], {"x": add(x, 1, 4)})
        for i in range(4):
            s = oacc[mine, i]
            for c in others:
                s = s + d2r[c, i].astype(F32)
            o3[g, i] = s
            d3s[g, i] = s.astype(BF16)
        for d in (1, 2, 3):
            t = add(zl, d, 4)
            send(d3s.at[g, t], d3r.at[g, d - 1], fS.at[g, d - 1], fR.at[g, d - 1], {"zl": t})

    def d4(g):
        s = tok[g * Q : (g + 1) * Q, :].astype(F32) + o3[g, zl]
        for d in (1, 2, 3):
            recv(d3r.at[g, d - 1], fS.at[g, d - 1], fR.at[g, d - 1], {"zl": add(zl, d, 4)})
            s = s + d3r[g, d - 1].astype(F32)
        out[g * Q : (g + 1) * Q, :] = s.astype(BF16)

    weights = []
    ops = (a1, a2, a3, mm, p2, zsend, hid, cy, cf, dn, d2, d3, d4, s1, s2, s3, s4)
    for o in ORDER:
        ops[o // 16](o % 16)
    for c in pending:
        c.wait_send()


def shards(tokens, norm_gain, gate_proj, up_proj, down_proj):
    T, DB = tokens.shape
    F = gate_proj.shape[1]
    Q = T // G
    PR, ZR, H, N = Q, Q // 2, 16, 8
    vmem = pl.BlockSpec(memory_space=pltpu.VMEM)
    hbm = pl.BlockSpec(memory_space=pl.ANY)
    dma = pltpu.SemaphoreType.DMA
    return pl.pallas_call(
        body,
        out_shape=jax.ShapeDtypeStruct((T, DB), BF16),
        in_specs=[hbm, hbm, hbm, hbm, hbm],
        out_specs=vmem,
        scratch_shapes=[
            pltpu.VMEM((T, DB), BF16),
            pltpu.VMEM((DB,), BF16),
            pltpu.VMEM((DB, 2 * F), BF16),
            pltpu.VMEM((F, DB), BF16),
            pltpu.VMEM((8, 8, 128), F32),
            pltpu.VMEM((2, 4, 4, 8, 128), F32),
            pltpu.VMEM((2, 4, G, 2, ZR, 128), F32),
            pltpu.VMEM((G, 4, 2, 4, Q, DB), BF16),
            pltpu.VMEM((H, 4, PR, 2 * F), BF16),
            pltpu.VMEM((H, 2, PR, F), BF16),
            pltpu.VMEM((H, 2, PR, 2 * F), BF16),
            pltpu.VMEM((H, ZR, 2 * F), BF16),
            pltpu.VMEM((H, ZR, 2 * F), BF16),
            pltpu.VMEM((H, 4, 2, ZR, F), BF16),
            pltpu.VMEM((N, 4, Q, DB), F32),
            pltpu.VMEM((N, 4, Q, DB), BF16),
            pltpu.VMEM((N, 4, Q, DB), BF16),
            pltpu.VMEM((N, 4, Q, DB), BF16),
            pltpu.VMEM((N, 4, Q, DB), BF16),
            pltpu.VMEM((G, 4, Q, DB), F32),
            pltpu.VMEM((G, 4, Q, DB), BF16),
            pltpu.VMEM((G, 3, Q, DB), BF16),
            dma((5,)),
            dma((8,)),
            dma((8,)),
            dma((7,)),
            dma((7,)),
            dma((G, 19)),
            dma((G, 19)),
            dma((H, 5)),
            dma((H, 5)),
            dma((H, 5)),
            dma((H, 5)),
            dma((N, 2)),
            dma((N, 2)),
            dma((G, 3)),
            dma((G, 3)),
        ],
        compiler_params=pltpu.CompilerParams(
            collective_id=0, has_side_effects=True, vmem_limit_bytes=60 * 2**20
        ),
        name="ffn",
    )(tokens, norm_gain, gate_proj, up_proj, down_proj)


def solution(mesh):
    split = Mesh(mesh.devices.reshape(4, 4, 2, 2, 4), ROW + COL)
    return jax.shard_map(
        shards,
        mesh=split,
        in_specs=(P(ROW, COL), P(COL), P(COL, ROW), P(COL, ROW), P(ROW, COL)),
        out_specs=P(ROW, COL),
        check_vma=False,
    )
```

```python
import jax
import jax.numpy as jnp
from jax import lax
from jax.experimental import pallas as pl
from jax.experimental.pallas import tpu as pltpu
from jax.sharding import Mesh
from jax.sharding import PartitionSpec as P

D = 8192
EPS = 0.25
MESH = pl.DeviceIdType.MESH
ROW = ("zl", "x", "core")
COL = ("zh", "y")

G = 2
DX = ((0, 1, 3, 2), (2, 3, 1, 0))
F32 = jnp.float32
BF16 = jnp.bfloat16

STEPS = (
    "a1", "a2", "a3", "mm", "p2", "zs", "hid", "cy", "cf", "dn", "d2", "d3", "d4", "s1", "s2", "s3", "s4",
)
ORDER = (
    1, 16, 48, 49, 208, 64, 33, 34, 65, 224, 51, 52, 53, 80, 50, 17, 240, 67, 81, 35,
    69, 68, 256, 96, 54, 83, 37, 85, 55, 38, 66, 60, 61, 70, 84, 97, 36, 57, 82, 71,
    58, 101, 77, 76, 59, 86, 100, 98, 56, 62, 87, 99, 74, 93, 92, 117, 75, 116, 103, 90,
    102, 63, 114, 109, 72, 91, 73, 133, 79, 119, 108, 78, 88, 89, 118, 130, 149, 115, 106, 107,
    95, 124, 132, 134, 135, 125, 112, 94, 104, 131, 148, 140, 105, 162, 122, 150, 113, 151, 146, 163,
    123, 147, 141, 111, 110, 156, 138, 120, 161, 121, 157, 139, 166, 129, 154, 136, 137, 128, 126, 155,
    165, 127, 145, 152, 153, 164, 144, 142, 160, 176, 143, 158, 159, 167, 177, 192, 193,
)


def own_half(j):
    return (j % 2 == 0) == (j < 8)


def body(
    tok_hbm, gain_hbm, gate, up, down, out,
    tok, gain, wgu, wd, sq, sg, sc, xg, part, r1, r2, zs, zr, hg, oacc, d1s, d1r, d2s, d2r, o3, d3s, d3r,
    wsem, sqS, sqR, eS, eR, aS, aR, bS, bR, cS, cR, dS, dR, fS, fR,
):
    zl, x, core, zh, y = [lax.axis_index(n) for n in ("zl", "x", "core", "zh", "y")]
    F = gate.shape[1]
    Q = tok.shape[0] // G
    PR, ZR, C = Q, Q // 2, 4 * Q
    col = zh * 4 + y

    def add(v, d, n):
        return lax.rem(v + d, n)

    yp, ym, y2 = add(y, 1, 4), add(y, 3, 4), add(y, 2, 4)

    t_copy = pltpu.make_async_copy(tok_hbm, tok, wsem.at[3])
    t_copy.start()
    g_copy = pltpu.make_async_copy(gain_hbm, gain, wsem.at[4])
    g_copy.start()
    w_copies = [
        pltpu.make_async_copy(gate, wgu.at[:, pl.ds(0, F)], wsem.at[0]),
        pltpu.make_async_copy(up, wgu.at[:, pl.ds(F, F)], wsem.at[1]),
        pltpu.make_async_copy(down, wd, wsem.at[2]),
    ]
    for c in w_copies:
        c.start()

    def colpeer(d):
        t = add(col, d, 8)
        return {"zh": t // 4, "y": lax.rem(t, 4)}

    peers = [colpeer(d) for d in range(1, 8)]
    peers += [{"zl": add(zl, d, 4)} for d in (1, 2, 3)]
    peers += [{"x": add(x, d, 4)} for d in (1, 2, 3)]
    peers += [{"core": 1 - core}]
    barrier = pltpu.get_barrier_semaphore()
    for p in peers:
        pl.semaphore_signal(barrier, inc=1, device_id=p, device_id_type=MESH)

    pending = []

    def send(src, dst, ss, rs, dev):
        c = pltpu.make_async_remote_copy(
            src_ref=src, dst_ref=dst, send_sem=ss, recv_sem=rs, device_id=dev, device_id_type=MESH
        )
        c.start()
        pending.append(c)

    def recv(dst, ss, rs, dev):
        pltpu.make_async_remote_copy(
            src_ref=dst, dst_ref=dst, send_sem=ss, recv_sem=rs, device_id=dev, device_id_type=MESH
        ).wait_recv()

    t_copy.wait()
    g_copy.wait()
    gain_row = gain[...].reshape(1, -1).astype(F32)
    acc = jnp.zeros((tok.shape[0], 128), F32)
    for g in range(tok.shape[1] // 128):
        cols = slice(g * 128, (g + 1) * 128)
        v = tok[:, cols].astype(F32)
        acc = acc + v * v
        v = (v * gain_row[:, cols]).astype(BF16)
        for g2 in range(G):
            xg[g2, x, core, zl, :, cols] = v[g2 * Q : (g2 + 1) * Q]
    acc = jnp.concatenate([acc, jnp.zeros((128 - tok.shape[0], 128), F32)], axis=0)
    sq[col] = jnp.broadcast_to(jnp.sum(acc.T, axis=0, keepdims=True), (8, 128))
    pl.semaphore_wait(barrier, len(peers))

    def xsend(g, d, b):
        mine = xg.at[g, x, core, add(zl, b, 4)]
        i = 3 + 4 * (d - 1) + b
        send(mine, mine, aS.at[g, i], aR.at[g, i], {"x": add(x, d, 4)})

    def a1(g):
        mine = xg.at[g, x, core, zl]
        for d in (1, 2, 3):
            send(mine, mine, aS.at[g, d - 1], aR.at[g, d - 1], {"zl": add(zl, d, 4)})
        for d in (1, 3, 2):
            xsend(g, d, 0)

    a1(0)
    for d in range(1, 8):
        send(sq.at[col], sq.at[col], sqS.at[d], sqR.at[d], colpeer(d))

    def s1(_):
        for d in range(1, 8):
            t = add(col, 8 - d, 8)
            recv(sq.at[t], sqS.at[d], sqR.at[d], colpeer(d))
        total = sq[0]
        for c in range(1, 8):
            total = total + sq[c]
        sg[core, x, zl] = 1.0 / jnp.sqrt(total / D + EPS)
        mine = sg.at[core, x, zl]
        for d in (1, 2, 3):
            send(mine, mine, eS.at[d - 1], eR.at[d - 1], {"zl": add(zl, d, 4)})

    def s2(_):
        for d in (1, 2, 3):
            s = add(zl, 4 - d, 4)
            recv(sg.at[core, x, s], eS.at[d - 1], eR.at[d - 1], {"zl": s})
        mine = sg.at[core, x]
        for d in (1, 2, 3):
            send(mine, mine, eS.at[d + 2], eR.at[d + 2], {"x": add(x, d, 4)})

    def s3(_):
        for d in (1, 2, 3):
            s = add(x, 4 - d, 4)
            recv(sg.at[core, s], eS.at[d + 2], eR.at[d + 2], {"x": s})
        mine = sg.at[core]
        send(mine, mine, eS.at[6], eR.at[6], {"core": 1 - core})

    def s4(_):
        recv(sg.at[1 - core], eS.at[6], eR.at[6], {"core": 1 - core})
        for h in (0, 1):
            for dx in range(4):
                v = jnp.broadcast_to(sg[h, add(x, dx, 4), y][0:1, :], (128, 128)).T
                sc[h, dx] = v[: G * Q, :].reshape(G, 2, ZR, 128)

    def a2(g):
        for d in (1, 2, 3):
            t = add(zl, 4 - d, 4)
            recv(xg.at[g, x, core, t], aS.at[g, d - 1], aR.at[g, d - 1], {"zl": t})
        mine = xg.at[g, x, core]
        send(mine, mine, aS.at[g, 15], aR.at[g, 15], {"core": 1 - core})
        for b in (1, 2, 3):
            for d in (1, 3, 2):
                xsend(g, d, b)

    def a3(c):
        g, dx = c // 4, DX[c // 4][c % 4]
        src, d = add(x, dx, 4), 4 - dx
        for b in range(4):
            i = 3 + 4 * (d - 1) + b
            recv(xg.at[g, src, core, add(zl, b, 4)], aS.at[g, i], aR.at[g, i], {"x": src})
        mine = xg.at[g, src, core]
        send(mine, mine, aS.at[g, 15 + dx], aR.at[g, 15 + dx], {"core": 1 - core})

    def mm(j):
        g, dx = j // 8, DX[j // 8][j // 2 % 4]
        src = add(x, dx, 4)
        half = core if own_half(j) else 1 - core
        if not own_half(j):
            recv(xg.at[g, src, half], aS.at[g, 15 + dx], aR.at[g, 15 + dx], {"core": 1 - core})
        if not weights:
            weights.append(True)
            w_copies[0].wait()
            w_copies[1].wait()

        def tile(n, carry):
            cols = pl.ds(pl.multiple_of(n * 256, 256), 256)
            r = jnp.dot(
                xg[g, src, half].reshape(C, xg.shape[-1]), wgu[:, cols], preferred_element_type=F32
            )
            part[j, :, :, cols] = r.astype(BF16).reshape(4, PR, 256)
            return carry

        lax.fori_loop(0, 2 * F // 256, tile, 0, unroll=True)
        send(part.at[j, y2, :, pl.ds(0, F)], r1.at[j, 0], bS.at[j, 0], bR.at[j, 0], {"y": yp})
        send(part.at[j, y2, :, pl.ds(F, F)], r1.at[j, 1], bS.at[j, 1], bR.at[j, 1], {"y": ym})

    def p2(j):
        recv(r1.at[j, 0], bS.at[j, 0], bR.at[j, 0], {"y": ym})
        a = part[j, yp, :, :F].astype(F32) + r1[j, 0].astype(F32)
        part[j, yp, :, :F] = a.astype(BF16)
        send(part.at[j, yp], r2.at[j, 0], bS.at[j, 2], bR.at[j, 2], {"y": yp})
        recv(r1.at[j, 1], bS.at[j, 1], bR.at[j, 1], {"y": yp})
        a = part[j, ym, :, F:].astype(F32) + r1[j, 1].astype(F32)
        part[j, ym, :, F:] = a.astype(BF16)
        send(part.at[j, ym], r2.at[j, 1], bS.at[j, 3], bR.at[j, 3], {"y": ym})

    def ysum(j, z, cols):
        rows = pl.ds(pl.multiple_of(z * ZR, ZR), ZR)
        s = part[j, y, rows, cols].astype(F32)
        return s + r2[j, 0, rows, cols].astype(F32) + r2[j, 1, rows, cols].astype(F32)

    def zsend(j):
        recv(r2.at[j, 0], bS.at[j, 2], bR.at[j, 2], {"y": ym})
        recv(r2.at[j, 1], bS.at[j, 3], bR.at[j, 3], {"y": yp})
        for cols in (slice(0, F), slice(F, 2 * F)):
            zs[j, :, cols] = ysum(j, 1 - zh, cols).astype(BF16)
        send(zs.at[j], zr.at[j], bS.at[j, 4], bR.at[j, 4], {"zh": 1 - zh})

    def hid(j):
        recv(zr.at[j], bS.at[j, 4], bR.at[j, 4], {"zh": 1 - zh})
        g = ysum(j, zh, slice(0, F)) + zr[j, :, :F].astype(F32)
        u = ysum(j, zh, slice(F, 2 * F)) + zr[j, :, F:].astype(F32)
        g2, dx = j // 8, DX[j // 8][j // 2 % 4]
        scale = sc[core if own_half(j) else 1 - core, dx, g2, zh][:, 0:1]
        g = g * scale
        u = u * scale
        hg[j, y, zh] = (jax.nn.silu(g) * u).astype(BF16)
        mine = hg.at[j, y, zh]
        send(mine, mine, cS.at[j, 0], cR.at[j, 0], {"zh": 1 - zh})

    def cy(j):
        recv(hg.at[j, y, 1 - zh], cS.at[j, 0], cR.at[j, 0], {"zh": 1 - zh})
        mine = hg.at[j, y]
        send(mine, mine, cS.at[j, 1], cR.at[j, 1], {"y": yp})
        send(mine, mine, cS.at[j, 2], cR.at[j, 2], {"y": ym})

    def cf(j):
        recv(hg.at[j, ym], cS.at[j, 1], cR.at[j, 1], {"y": ym})
        send(hg.at[j, ym, 0], hg.at[j, ym, 0], cS.at[j, 3], cR.at[j, 3], {"y": yp})
        recv(hg.at[j, yp], cS.at[j, 2], cR.at[j, 2], {"y": yp})
        send(hg.at[j, yp, 1], hg.at[j, yp, 1], cS.at[j, 4], cR.at[j, 4], {"y": ym})

    def dn(j):
        k = j // 2
        recv(hg.at[j, y2, 0], cS.at[j, 3], cR.at[j, 3], {"y": ym})
        recv(hg.at[j, y2, 1], cS.at[j, 4], cR.at[j, 4], {"y": yp})
        if len(weights) == 1:
            weights.append(True)
            w_copies[2].wait()

        def tile(n, carry):
            cols = pl.ds(pl.multiple_of(n * 256, 256), 256)
            r = jnp.dot(hg[j].reshape(C, F), wd[:, cols], preferred_element_type=F32)
            r = r.reshape(4, Q, 256)
            if own_half(j):
                oacc[k, :, :, cols] = r
            else:
                d1s[k, :, :, cols] = r.astype(BF16)
            return carry

        lax.fori_loop(0, wd.shape[1] // 256, tile, 0, unroll=True)
        if not own_half(j):
            send(d1s.at[k], d1r.at[k], dS.at[k, 0], dR.at[k, 0], {"core": 1 - core})

    def d2(c):
        dx = DX[c // 4][c % 4]
        recv(d1r.at[c], dS.at[c, 0], dR.at[c, 0], {"core": 1 - core})
        for i in range(4):
            s = oacc[c, i] + d1r[c, i].astype(F32)
            if dx:
                d2s[c, i] = s.astype(BF16)
            else:
                oacc[c, i] = s
        if dx:
            send(d2s.at[c], d2r.at[c], dS.at[c, 1], dR.at[c, 1], {"x": add(x, dx, 4)})

    def d3(g):
        mine = 4 * g + DX[g].index(0)
        others = [4 * g + i for i in range(4) if DX[g][i]]
        for c in others:
            recv(d2r.at[c], dS.at[c, 1], dR.at[c, 1], {"x": add(x, 1, 4)})
        for i in range(4):
            s = oacc[mine, i]
            for c in others:
                s = s + d2r[c, i].astype(F32)
            o3[g, i] = s
            d3s[g, i] = s.astype(BF16)
        for d in (1, 2, 3):
            t = add(zl, d, 4)
            send(d3s.at[g, t], d3r.at[g, d - 1], fS.at[g, d - 1], fR.at[g, d - 1], {"zl": t})

    def d4(g):
        s = tok[g * Q : (g + 1) * Q, :].astype(F32) + o3[g, zl]
        for d in (1, 2, 3):
            recv(d3r.at[g, d - 1], fS.at[g, d - 1], fR.at[g, d - 1], {"zl": add(zl, d, 4)})
            s = s + d3r[g, d - 1].astype(F32)
        out[g * Q : (g + 1) * Q, :] = s.astype(BF16)

    weights = []
    ops = (a1, a2, a3, mm, p2, zsend, hid, cy, cf, dn, d2, d3, d4, s1, s2, s3, s4)
    for o in ORDER:
        ops[o // 16](o % 16)
    for c in pending:
        c.wait_send()


def shards(tokens, norm_gain, gate_proj, up_proj, down_proj):
    T, DB = tokens.shape
    F = gate_proj.shape[1]
    Q = T // G
    PR, ZR, H, N = Q, Q // 2, 16, 8
    vmem = pl.BlockSpec(memory_space=pltpu.VMEM)
    hbm = pl.BlockSpec(memory_space=pl.ANY)
    dma = pltpu.SemaphoreType.DMA
    return pl.pallas_call(
        body,
        out_shape=jax.ShapeDtypeStruct((T, DB), BF16),
        in_specs=[hbm, hbm, hbm, hbm, hbm],
        out_specs=vmem,
        scratch_shapes=[
            pltpu.VMEM((T, DB), BF16),
            pltpu.VMEM((DB,), BF16),
            pltpu.VMEM((DB, 2 * F), BF16),
            pltpu.VMEM((F, DB), BF16),
            pltpu.VMEM((8, 8, 128), F32),
            pltpu.VMEM((2, 4, 4, 8, 128), F32),
            pltpu.VMEM((2, 4, G, 2, ZR, 128), F32),
            pltpu.VMEM((G, 4, 2, 4, Q, DB), BF16),
            pltpu.VMEM((H, 4, PR, 2 * F), BF16),
            pltpu.VMEM((H, 2, PR, F), BF16),
            pltpu.VMEM((H, 2, PR, 2 * F), BF16),
            pltpu.VMEM((H, ZR, 2 * F), BF16),
            pltpu.VMEM((H, ZR, 2 * F), BF16),
            pltpu.VMEM((H, 4, 2, ZR, F), BF16),
            pltpu.VMEM((N, 4, Q, DB), F32),
            pltpu.VMEM((N, 4, Q, DB), BF16),
            pltpu.VMEM((N, 4, Q, DB), BF16),
            pltpu.VMEM((N, 4, Q, DB), BF16),
            pltpu.VMEM((N, 4, Q, DB), BF16),
            pltpu.VMEM((G, 4, Q, DB), F32),
            pltpu.VMEM((G, 4, Q, DB), BF16),
            pltpu.VMEM((G, 3, Q, DB), BF16),
            dma((5,)),
            dma((8,)),
            dma((8,)),
            dma((7,)),
            dma((7,)),
            dma((G, 19)),
            dma((G, 19)),
            dma((H, 5)),
            dma((H, 5)),
            dma((H, 5)),
            dma((H, 5)),
            dma((N, 2)),
            dma((N, 2)),
            dma((G, 3)),
            dma((G, 3)),
        ],
        compiler_params=pltpu.CompilerParams(
            collective_id=0, has_side_effects=True, vmem_limit_bytes=60 * 2**20
        ),
        name="ffn",
    )(tokens, norm_gain, gate_proj, up_proj, down_proj)


def solution(mesh):
    split = Mesh(mesh.devices.reshape(4, 4, 2, 2, 4), ROW + COL)
    return jax.shard_map(
        shards,
        mesh=split,
        in_specs=(P(ROW, COL), P(COL), P(COL, ROW), P(COL, ROW), P(ROW, COL)),
        out_specs=P(ROW, COL),
        check_vma=False,
    )
```

```python
import jax
import jax.numpy as jnp
from jax import lax
from jax.experimental import pallas as pl
from jax.experimental.pallas import tpu as pltpu
from jax.sharding import Mesh
from jax.sharding import PartitionSpec as P

D = 8192
EPS = 0.25
MESH = pl.DeviceIdType.MESH
ROW = ("zl", "x", "core")
COL = ("zh", "y")

K = 8
F32 = jnp.float32
BF16 = jnp.bfloat16

STEPS = ("a2", "a3", "mm", "p2", "zs", "hid", "cy", "cf", "dn", "d2", "d3", "d4", "s1", "s2", "s3", "s4")
ORDER = (
    0, 1, 2, 192, 16, 32, 33, 17, 34, 5, 48, 4, 18, 49, 37, 21, 43, 50, 64, 208,
    20, 53, 6, 36, 41, 224, 7, 65, 35, 59, 42, 66, 40, 69, 240, 80, 22, 51, 52, 75,
    81, 56, 57, 82, 67, 3, 58, 68, 85, 23, 47, 46, 19, 73, 39, 91, 44, 72, 38, 96,
    45, 55, 84, 62, 89, 97, 112, 83, 54, 74, 61, 60, 88, 71, 78, 70, 113, 90, 100, 87,
    104, 76, 101, 129, 63, 128, 105, 86, 99, 120, 77, 103, 121, 117, 98, 79, 144, 116, 115, 136,
    106, 102, 94, 119, 92, 137, 148, 93, 132, 114, 133, 107, 146, 122, 131, 95, 118, 110, 130, 145,
    108, 123, 135, 109, 134, 126, 147, 124, 138, 111, 164, 162, 139, 125, 149, 160, 140, 142, 161, 127,
    141, 150, 180, 178, 143, 163, 151, 166, 177, 179, 165, 167, 181, 176, 182, 183,
)


def own_half(j):
    return (j % 2 == 0) == (j // 2 < K // 2)


def body(
    tok_hbm, gain_hbm, gate, up, down, out,
    tok, gain, wgu, wd, sq, sg, sc, xg, part, r1, r2, zs, zr, hg, oacc, d1s, d1r, d2s, d2r, o3, d3s, d3r,
    wsem, sqS, sqR, eS, eR, aS, aR, bS, bR, cS, cR, dS, dR,
):
    zl, x, core, zh, y = [lax.axis_index(n) for n in ("zl", "x", "core", "zh", "y")]
    F = gate.shape[1]
    R = tok.shape[0] // K
    PR, ZR, C = 4 * R, 2 * R, 16 * R
    col = zh * 4 + y

    def add(v, d, n):
        return lax.rem(v + d, n)

    yp, ym, y2 = add(y, 1, 4), add(y, 3, 4), add(y, 2, 4)

    t_copy = pltpu.make_async_copy(tok_hbm, tok, wsem.at[3])
    t_copy.start()
    g_copy = pltpu.make_async_copy(gain_hbm, gain, wsem.at[4])
    g_copy.start()
    w_copies = [
        pltpu.make_async_copy(gate, wgu.at[:, pl.ds(0, F)], wsem.at[0]),
        pltpu.make_async_copy(up, wgu.at[:, pl.ds(F, F)], wsem.at[1]),
        pltpu.make_async_copy(down, wd, wsem.at[2]),
    ]
    for c in w_copies:
        c.start()

    def colpeer(d):
        t = add(col, d, 8)
        return {"zh": t // 4, "y": lax.rem(t, 4)}

    peers = [colpeer(d) for d in range(1, 8)]
    peers += [{"zl": add(zl, d, 4)} for d in (1, 2, 3)]
    peers += [{"x": add(x, d, 4)} for d in (1, 2, 3)]
    peers += [{"core": 1 - core}]
    barrier = pltpu.get_barrier_semaphore()
    for p in peers:
        pl.semaphore_signal(barrier, inc=1, device_id=p, device_id_type=MESH)

    pending = []

    def send(src, dst, ss, rs, dev):
        c = pltpu.make_async_remote_copy(
            src_ref=src, dst_ref=dst, send_sem=ss, recv_sem=rs, device_id=dev, device_id_type=MESH
        )
        c.start()
        pending.append(c)

    def recv(dst, ss, rs, dev):
        pltpu.make_async_remote_copy(
            src_ref=dst, dst_ref=dst, send_sem=ss, recv_sem=rs, device_id=dev, device_id_type=MESH
        ).wait_recv()

    t_copy.wait()
    g_copy.wait()
    gain_row = gain[...].reshape(1, -1).astype(F32)
    acc = jnp.zeros((tok.shape[0], 128), F32)
    for g in range(tok.shape[1] // 128):
        cols = slice(g * 128, (g + 1) * 128)
        v = tok[:, cols].astype(F32)
        acc = acc + v * v
        v = (v * gain_row[:, cols]).astype(BF16)
        for k in range(K):
            xg[k, core, x, zl, :, cols] = v[k * R : (k + 1) * R]
    acc = jnp.concatenate([acc, jnp.zeros((128 - tok.shape[0], 128), F32)], axis=0)
    sq[col] = jnp.broadcast_to(jnp.sum(acc.T, axis=0, keepdims=True), (8, 128))
    pl.semaphore_wait(barrier, len(peers))

    def a1(k):
        mine = xg.at[k, core, x, zl]
        for d in (1, 2, 3):
            send(mine, mine, aS.at[k, d - 1], aR.at[k, d - 1], {"zl": add(zl, d, 4)})

    a1(0)
    for d in range(1, 8):
        send(sq.at[col], sq.at[col], sqS.at[d], sqR.at[d], colpeer(d))
    for k in range(1, K):
        a1(k)

    def s1(_):
        for d in range(1, 8):
            t = add(col, 8 - d, 8)
            recv(sq.at[t], sqS.at[d], sqR.at[d], colpeer(d))
        total = sq[0]
        for c in range(1, 8):
            total = total + sq[c]
        sg[core, x, zl] = 1.0 / jnp.sqrt(total / D + EPS)
        mine = sg.at[core, x, zl]
        for d in (1, 2, 3):
            send(mine, mine, eS.at[d - 1], eR.at[d - 1], {"zl": add(zl, d, 4)})

    def s2(_):
        for d in (1, 2, 3):
            s = add(zl, 4 - d, 4)
            recv(sg.at[core, x, s], eS.at[d - 1], eR.at[d - 1], {"zl": s})
        mine = sg.at[core, x]
        for d in (1, 2, 3):
            send(mine, mine, eS.at[d + 2], eR.at[d + 2], {"x": add(x, d, 4)})

    def s3(_):
        for d in (1, 2, 3):
            s = add(x, 4 - d, 4)
            recv(sg.at[core, s], eS.at[d + 2], eR.at[d + 2], {"x": s})
        mine = sg.at[core]
        send(mine, mine, eS.at[6], eR.at[6], {"core": 1 - core})

    def s4(_):
        recv(sg.at[1 - core], eS.at[6], eR.at[6], {"core": 1 - core})
        for h in (0, 1):
            for i in (0, 1):
                v = jnp.broadcast_to(sg[h, y, 2 * zh + i][0:1, :], (128, 128)).T
                sc[h, :, i] = v[: K * R, :].reshape(K, R, 128)

    def a2(k):
        for d in (1, 2, 3):
            s = add(zl, 4 - d, 4)
            recv(xg.at[k, core, x, s], aS.at[k, d - 1], aR.at[k, d - 1], {"zl": s})
        mine = xg.at[k, core, x]
        for d in (1, 2, 3):
            send(mine, mine, aS.at[k, d + 2], aR.at[k, d + 2], {"x": add(x, d, 4)})

    def a3(k):
        for d in (1, 2, 3):
            s = add(x, 4 - d, 4)
            recv(xg.at[k, core, s], aS.at[k, d + 2], aR.at[k, d + 2], {"x": s})
        mine = xg.at[k, core]
        send(mine, mine, aS.at[k, 6], aR.at[k, 6], {"core": 1 - core})

    def mm(j):
        k = j // 2
        half = core if own_half(j) else 1 - core
        if not own_half(j):
            recv(xg.at[k, half], aS.at[k, 6], aR.at[k, 6], {"core": 1 - core})
        if not weights:
            weights.append(True)
            w_copies[0].wait()
            w_copies[1].wait()

        def tile(n, carry):
            cols = pl.ds(pl.multiple_of(n * 256, 256), 256)
            r = jnp.dot(
                xg[k, half].reshape(C, xg.shape[-1]), wgu[:, cols], preferred_element_type=F32
            )
            part[j, :, :, cols] = r.astype(BF16).reshape(4, PR, 256)
            return carry

        lax.fori_loop(0, 2 * F // 256, tile, 0, unroll=True)
        send(part.at[j, y2, :, pl.ds(0, F)], r1.at[j, 0], bS.at[j, 0], bR.at[j, 0], {"y": yp})
        send(part.at[j, y2, :, pl.ds(F, F)], r1.at[j, 1], bS.at[j, 1], bR.at[j, 1], {"y": ym})

    def p2(j):
        recv(r1.at[j, 0], bS.at[j, 0], bR.at[j, 0], {"y": ym})
        a = part[j, yp, :, :F].astype(F32) + r1[j, 0].astype(F32)
        part[j, yp, :, :F] = a.astype(BF16)
        send(part.at[j, yp], r2.at[j, 0], bS.at[j, 2], bR.at[j, 2], {"y": yp})
        recv(r1.at[j, 1], bS.at[j, 1], bR.at[j, 1], {"y": yp})
        a = part[j, ym, :, F:].astype(F32) + r1[j, 1].astype(F32)
        part[j, ym, :, F:] = a.astype(BF16)
        send(part.at[j, ym], r2.at[j, 1], bS.at[j, 3], bR.at[j, 3], {"y": ym})

    def ysum(j, z, cols):
        rows = pl.ds(pl.multiple_of(z * ZR, ZR), ZR)
        s = part[j, y, rows, cols].astype(F32)
        return s + r2[j, 0, rows, cols].astype(F32) + r2[j, 1, rows, cols].astype(F32)

    def zsend(j):
        recv(r2.at[j, 0], bS.at[j, 2], bR.at[j, 2], {"y": ym})
        recv(r2.at[j, 1], bS.at[j, 3], bR.at[j, 3], {"y": yp})
        for cols in (slice(0, F), slice(F, 2 * F)):
            zs[j, :, cols] = ysum(j, 1 - zh, cols).astype(BF16)
        send(zs.at[j], zr.at[j], bS.at[j, 4], bR.at[j, 4], {"zh": 1 - zh})

    def hid(j):
        recv(zr.at[j], bS.at[j, 4], bR.at[j, 4], {"zh": 1 - zh})
        g = ysum(j, zh, slice(0, F)) + zr[j, :, :F].astype(F32)
        u = ysum(j, zh, slice(F, 2 * F)) + zr[j, :, F:].astype(F32)
        k = j // 2
        scale = sc[core if own_half(j) else 1 - core, k].reshape(ZR, 128)[:, 0:1]
        g = g * scale
        u = u * scale
        hg[j, y, zh] = (jax.nn.silu(g) * u).astype(BF16)
        mine = hg.at[j, y, zh]
        send(mine, mine, cS.at[j, 0], cR.at[j, 0], {"zh": 1 - zh})

    def cy(j):
        recv(hg.at[j, y, 1 - zh], cS.at[j, 0], cR.at[j, 0], {"zh": 1 - zh})
        mine = hg.at[j, y]
        send(mine, mine, cS.at[j, 1], cR.at[j, 1], {"y": yp})
        send(mine, mine, cS.at[j, 2], cR.at[j, 2], {"y": ym})

    def cf(j):
        recv(hg.at[j, ym], cS.at[j, 1], cR.at[j, 1], {"y": ym})
        send(hg.at[j, ym, 0], hg.at[j, ym, 0], cS.at[j, 3], cR.at[j, 3], {"y": yp})
        recv(hg.at[j, yp], cS.at[j, 2], cR.at[j, 2], {"y": yp})
        send(hg.at[j, yp, 1], hg.at[j, yp, 1], cS.at[j, 4], cR.at[j, 4], {"y": ym})

    def dn(j):
        k = j // 2
        recv(hg.at[j, y2, 0], cS.at[j, 3], cR.at[j, 3], {"y": ym})
        recv(hg.at[j, y2, 1], cS.at[j, 4], cR.at[j, 4], {"y": yp})
        if len(weights) == 1:
            weights.append(True)
            w_copies[2].wait()

        def tile(n, carry):
            cols = pl.ds(pl.multiple_of(n * 256, 256), 256)
            r = jnp.dot(hg[j].reshape(C, F), wd[:, cols], preferred_element_type=F32)
            r = r.reshape(4, 4 * R, 256)
            if own_half(j):
                oacc[k, :, :, cols] = r
            else:
                d1s[k, :, :, cols] = r.astype(BF16)
            return carry

        lax.fori_loop(0, wd.shape[1] // 256, tile, 0, unroll=True)
        if not own_half(j):
            send(d1s.at[k], d1r.at[k], dS.at[k, 0], dR.at[k, 0], {"core": 1 - core})

    def d2(k):
        recv(d1r.at[k], dS.at[k, 0], dR.at[k, 0], {"core": 1 - core})
        for i in range(4):
            s = oacc[k, i] + d1r[k, i].astype(F32)
            oacc[k, i] = s
            d2s[k, i] = s.astype(BF16)
        for d in (1, 2, 3):
            t = add(x, d, 4)
            send(d2s.at[k, t], d2r.at[k, d - 1], dS.at[k, d], dR.at[k, d], {"x": t})

    def d3(k):
        s = oacc[k, x]
        for d in (1, 2, 3):
            recv(d2r.at[k, d - 1], dS.at[k, d], dR.at[k, d], {"x": add(x, d, 4)})
            s = s + d2r[k, d - 1].astype(F32)
        s = s.reshape(4, R, s.shape[-1])
        o3[k] = s
        d3s[k] = s.astype(BF16)
        for d in (1, 2, 3):
            t = add(zl, d, 4)
            send(d3s.at[k, t], d3r.at[k, d - 1], dS.at[k, d + 3], dR.at[k, d + 3], {"zl": t})

    def d4(k):
        s = tok[k * R : (k + 1) * R, :].astype(F32) + o3[k, zl]
        for d in (1, 2, 3):
            recv(d3r.at[k, d - 1], dS.at[k, d + 3], dR.at[k, d + 3], {"zl": add(zl, d, 4)})
            s = s + d3r[k, d - 1].astype(F32)
        out[k * R : (k + 1) * R, :] = s.astype(BF16)

    weights = []
    ops = (a2, a3, mm, p2, zsend, hid, cy, cf, dn, d2, d3, d4, s1, s2, s3, s4)
    for o in ORDER:
        ops[o // 16](o % 16)
    for c in pending:
        c.wait_send()


def shards(tokens, norm_gain, gate_proj, up_proj, down_proj):
    T, DB = tokens.shape
    F = gate_proj.shape[1]
    R = T // K
    PR, ZR, H = 4 * R, 2 * R, 2 * K
    vmem = pl.BlockSpec(memory_space=pltpu.VMEM)
    hbm = pl.BlockSpec(memory_space=pl.ANY)
    dma = pltpu.SemaphoreType.DMA
    return pl.pallas_call(
        body,
        out_shape=jax.ShapeDtypeStruct((T, DB), BF16),
        in_specs=[hbm, hbm, hbm, hbm, hbm],
        out_specs=vmem,
        scratch_shapes=[
            pltpu.VMEM((T, DB), BF16),
            pltpu.VMEM((DB,), BF16),
            pltpu.VMEM((DB, 2 * F), BF16),
            pltpu.VMEM((F, DB), BF16),
            pltpu.VMEM((8, 8, 128), F32),
            pltpu.VMEM((2, 4, 4, 8, 128), F32),
            pltpu.VMEM((2, K, 2, R, 128), F32),
            pltpu.VMEM((K, 2, 4, 4, R, DB), BF16),
            pltpu.VMEM((H, 4, PR, 2 * F), BF16),
            pltpu.VMEM((H, 2, PR, F), BF16),
            pltpu.VMEM((H, 2, PR, 2 * F), BF16),
            pltpu.VMEM((H, ZR, 2 * F), BF16),
            pltpu.VMEM((H, ZR, 2 * F), BF16),
            pltpu.VMEM((H, 4, 2, ZR, F), BF16),
            pltpu.VMEM((K, 4, 4 * R, DB), F32),
            pltpu.VMEM((K, 4, 4 * R, DB), BF16),
            pltpu.VMEM((K, 4, 4 * R, DB), BF16),
            pltpu.VMEM((K, 4, 4 * R, DB), BF16),
            pltpu.VMEM((K, 3, 4 * R, DB), BF16),
            pltpu.VMEM((K, 4, R, DB), F32),
            pltpu.VMEM((K, 4, R, DB), BF16),
            pltpu.VMEM((K, 3, R, DB), BF16),
            dma((5,)),
            dma((8,)),
            dma((8,)),
            dma((7,)),
            dma((7,)),
            dma((K, 7)),
            dma((K, 7)),
            dma((H, 5)),
            dma((H, 5)),
            dma((H, 5)),
            dma((H, 5)),
            dma((K, 7)),
            dma((K, 7)),
        ],
        compiler_params=pltpu.CompilerParams(
            collective_id=0, has_side_effects=True, vmem_limit_bytes=60 * 2**20
        ),
        name="ffn",
    )(tokens, norm_gain, gate_proj, up_proj, down_proj)


def solution(mesh):
    split = Mesh(mesh.devices.reshape(4, 4, 2, 2, 4), ROW + COL)
    return jax.shard_map(
        shards,
        mesh=split,
        in_specs=(P(ROW, COL), P(COL), P(COL, ROW), P(COL, ROW), P(ROW, COL)),
        out_specs=P(ROW, COL),
        check_vma=False,
    )
```
